256 devices in a mesh: groups: 2 (over y), seq: 16 (over z), batch: 4 (over x), head: 2 (over core).
Axes of the slice: x: 4, y: 2, z: 16, core: 2. Of those that a mesh axis runs over, the one named last changes fastest.
The devices are a block of a 4x16x16 slice.
Arguments:
- hidden_in: bfloat16 [128, 4096], P(('groups', 'batch'), 'seq'), parts along dimension 0, may hold values from -400 to 400
- norm_gain_vector: bfloat16 [4096], P('seq'), may hold values from 0.099609375 to 1.8984375
- w_query: bfloat16 [4096, 4096], P('seq', 'head'), may hold values from -0.09375 to 0.09375
- key_cache_rows: bfloat16 [128, 16384, 128], P(('groups', 'batch'), 'seq'), parts along dimension 0, may hold values from -360 to 360
- value_cache_rows: bfloat16 [128, 16384, 128], P(('groups', 'batch'), 'seq'), parts along dimension 0, may hold values from -6 to 6
- k_new: bfloat16 [128, 128], P(('groups', 'batch')), parts along dimension 0, may hold values from -360 to 360
- v_new: bfloat16 [128, 128], P(('groups', 'batch')), parts along dimension 0, may hold values from -6 to 6
- lengths: int32 [128], P(('groups', 'batch')), parts along dimension 0, may hold values from 1 to 16384, as said below
- w_out: bfloat16 [4096, 4096], P('head', 'seq'), may hold values from -0.09375 to 0.09375
Outputs:
- layer_out: float32 [128, 4096], P(('groups', 'batch'), ('seq', 'head')), parts along dimension 0
The draws below stay inside these ranges and needn't reach their ends.
There are 2 independent parts, one for each index of `groups`. The reference program is written for one: setup_inputs(seed, part) draws one part's arguments, and reference() takes and returns one part's arrays. A program takes and returns all parts, laid end to end along the dimension named above; an argument that names none is the same for every part. Nothing has to cross between parts.
Inputs may be any that keep to these rules, and one draw needn't show every extreme that they name: `lengths`: every sequence has at least one cached position; some sequence of each draw uses all 16384.
All inputs are finite; a program needn't handle non-finite values.
Results may differ from the reference program's by a relative error of at most 0.008.
Values sent between devices are 32-bit elements; how exact they have to be, the bound alone decides.
No kernel may reach another device: no remote copies, remote signals or barrier semaphores. Data moves between devices by JAX's collectives and lax.ppermute only.
A program may use at most 64 MiB of HBM per device.

```python
import jax
import jax.numpy as jnp
from jax import lax

D = 4096
HQ = 32
HD = 128
B = 64
CTX = 16384
QW = 4096


def drawn_keys(key, shape):
    values = jnp.clip(jax.random.normal(key, shape, jnp.float32), -6.0, 6.0) * 2.5
    return values


def draw_key_cache_rows(key, part):
    values = drawn_keys(jax.random.fold_in(key, 1), (B, CTX, HD))
    return values.astype(jnp.bfloat16)


def draw_k_new(key, part):
    values = drawn_keys(jax.random.fold_in(key, 2), (B, HD))
    return values.astype(jnp.bfloat16)


def draw_hidden_in(key, part):
    first, second, third = jax.random.split(jax.random.fold_in(key, 3), 3)
    base = jnp.clip(jax.random.normal(first, (B, D), jnp.float32), -4.0, 4.0)
    row_scale = jnp.exp(jax.random.uniform(second, (B, 1), jnp.float32) * jnp.log(10.0))
    ramp = jnp.arange(D, dtype=jnp.float32)[None, :] / D
    power = 0.24 * ramp + 0.76 * jax.random.uniform(third, (1, D), jnp.float32)
    col_scale = jnp.exp(power * jnp.log(10.0))
    return (base * row_scale * col_scale).astype(jnp.bfloat16)


def draw_lengths(key, part):
    first, second = jax.random.split(jax.random.fold_in(key, 4))
    values = jax.random.randint(first, (B,), 1, CTX + 1, jnp.int32)
    chosen = jax.random.randint(second, (), 0, B, jnp.int32)
    return jnp.where(jnp.arange(B, dtype=jnp.int32) == chosen, CTX, values).astype(jnp.int32)


def block_scale(stream_key, extent, cuts, least, top_value):
    level = 1.0
    for dim, blocks in cuts:
        steps = jax.random.uniform(jax.random.fold_in(jax.random.fold_in(stream_key, 6), dim), (blocks,), jnp.float32, least / len(cuts), top_value / len(cuts))
        level = level * jnp.repeat(jnp.exp(steps), extent[dim] // blocks).reshape((-1,) + (1,) * (len(extent) - 1 - dim))
    return level


def bell_draw(key, shape, scale, limit, shards=(), kind=jnp.bfloat16):
    gain = block_scale(key, shape, shards, -0.22, 0.18) if shards else 1.0
    entries = jax.random.normal(key, shape, jnp.float32) * scale * gain
    return jnp.minimum(jnp.maximum(entries, -limit), limit).astype(kind)


def setup_inputs(seed: int = 0, part: int = 0) -> dict:
    key_list = jax.random.split(jax.random.key(seed), 10)
    part_keys = jax.random.split(jax.random.fold_in(key_list[9], part), 10)
    hidden_in = draw_hidden_in(jax.random.fold_in(jax.random.fold_in(key_list[9], part), 71), part)
    norm_gain_vector = jnp.clip(1.0 + 0.18 * jax.random.normal(key_list[1], (D,), jnp.float32), 0.099609375, 1.8984375).astype(jnp.bfloat16)
    w_query = bell_draw(key_list[2], (D, QW), D ** -0.5, 0.09375, ((0, 16), (1, 2)))
    key_cache_rows = draw_key_cache_rows(jax.random.fold_in(jax.random.fold_in(key_list[9], part), 71), part)
    value_cache_rows = bell_draw(part_keys[4], (B, CTX, HD), 1.0, 6.0, ((0, 4), (1, 16)))
    k_new = draw_k_new(jax.random.fold_in(jax.random.fold_in(key_list[9], part), 71), part)
    v_new = bell_draw(part_keys[6], (B, HD), 1.0, 6.0, ((0, 4),))
    lengths = draw_lengths(jax.random.fold_in(jax.random.fold_in(key_list[9], part), 71), part)
    w_out = bell_draw(key_list[8], (QW, D), QW ** -0.5, 0.09375, ((0, 2), (1, 16)))
    return dict(hidden_in=hidden_in, norm_gain_vector=norm_gain_vector, w_query=w_query, key_cache_rows=key_cache_rows, value_cache_rows=value_cache_rows, k_new=k_new, v_new=v_new, lengths=lengths, w_out=w_out)


def reference(hidden_in, norm_gain_vector, w_query, key_cache_rows, value_cache_rows, k_new, v_new, lengths, w_out):
    inputs = hidden_in.astype(jnp.float32)
    mean_sq = lax.optimization_barrier(jnp.mean(inputs * inputs, axis=-1, keepdims=True))
    normed = (inputs * lax.rsqrt(mean_sq + 1e-05) * norm_gain_vector.astype(jnp.float32)).astype(jnp.bfloat16)
    inverse_root_norm = 1.0 / HD ** 0.5
    query_vectors = (jnp.dot(normed, w_query, preferred_element_type=jnp.float32) * inverse_root_norm).astype(jnp.bfloat16)
    query_vectors = query_vectors.reshape(query_vectors.shape[0], HQ, HD)

    def attend(per_seq):
        query_rows, key_rows, value_rows, used, key_own, value_own = per_seq
        scores = jnp.dot(query_rows, key_rows.T, preferred_element_type=jnp.float32)
        own = jnp.dot(query_rows, key_own, preferred_element_type=jnp.float32)
        live_mask = lax.iota(jnp.int32, key_rows.shape[0]) < used
        top = jnp.maximum(lax.optimization_barrier(jnp.max(jnp.where(live_mask[None, :], scores, -jnp.inf), axis=-1)), own)
        softmax_weights = jnp.where(live_mask[None, :], jnp.exp(scores - top[:, None]), jnp.float32(0.0))
        fresh = jnp.exp(own - top)
        totals = lax.optimization_barrier(jnp.sum(softmax_weights, axis=-1)) + fresh
        summed = jnp.dot(softmax_weights.astype(jnp.bfloat16), value_rows, preferred_element_type=jnp.float32)
        result = (summed + fresh[:, None] * value_own.astype(jnp.float32)[None, :]) / totals[:, None]
        return result.astype(jnp.bfloat16).reshape(HQ * HD)
    attended = lax.map(attend, (query_vectors, key_cache_rows, value_cache_rows, lengths, k_new, v_new))
    return jnp.dot(attended, w_out, preferred_element_type=jnp.float32)
```

```python
import functools

import jax
import jax.numpy as jnp
from jax import lax
from jax.experimental import pallas as pl
from jax.experimental.pallas import tpu as pltpu
from jax.sharding import PartitionSpec as P

HD = 128
FLOOR = -1e30
F32 = jnp.float32
BF16 = jnp.bfloat16


def exchanged(blocks, axis):
    return lax.all_to_all(blocks, axis, split_axis=0, concat_axis=0, tiled=True)


def swapped(array, axis):
    return lax.ppermute(array, axis, [(0, 1), (1, 0)])


def call(kernel, shapes, *args, smem=(), mib=16):
    spaces = [pltpu.SMEM if i in smem else pltpu.VMEM for i in range(len(args))]
    return pl.pallas_call(
        kernel,
        out_shape=[jax.ShapeDtypeStruct(s, F32) for s in shapes],
        in_specs=[pl.BlockSpec(memory_space=s) for s in spaces],
        out_specs=[pl.BlockSpec(memory_space=pltpu.VMEM) for _ in shapes],
        compiler_params=pltpu.CompilerParams(vmem_limit_bytes=mib << 20),
    )(*args)


def project(x_ref, g_ref, w_ref, out_ref):
    rows = x_ref.shape[0]
    x = x_ref[...].astype(F32)
    squares = jnp.sum(x * x, axis=1, keepdims=True)
    scaled = x * g_ref[...].astype(F32)
    high = scaled.astype(BF16)
    low = (scaled - high.astype(F32)).astype(BF16)
    both = jnp.concatenate([high, low], axis=0)
    part = jnp.dot(both, w_ref[...], preferred_element_type=F32)
    part = part[:rows] + part[rows:]
    heads = part.shape[1] // HD
    for h in range(heads):
        out_ref[:, h, :] = part[:, h * HD : (h + 1) * HD]
    out_ref[:, heads, :] = jnp.broadcast_to(squares, (rows, HD))


def finish_query(features, got_ref, all_ref, mine_ref):
    n, _, _ = got_ref.shape
    heads = mine_ref.shape[0]
    total = got_ref[0]
    for i in range(1, n):
        total = total + got_ref[i]
    scale = lax.rsqrt(total[heads : heads + 1] / features + 1e-05)
    root = 1.0 / HD**0.5
    mine = (total[:heads] * scale * root).astype(BF16).astype(F32)
    mine_ref[...] = mine
    for i in range(n):
        all_ref[i] = mine


def attend(q_ref, k_ref, v_ref, len_ref, out_ref):
    rows, heads, _ = q_ref.shape
    block = k_ref.shape[1]
    start = lax.axis_index("seq") * block
    at = start + lax.broadcasted_iota(jnp.int32, (heads, block), 1)
    lane = lax.broadcasted_iota(jnp.int32, (heads, HD), 1)
    tops = jnp.zeros((heads, HD), F32)
    totals = jnp.zeros((heads, HD), F32)
    for b in range(rows):
        q = q_ref[b].astype(BF16)
        s = lax.dot_general(q, k_ref[b], (((1,), (1,)), ((), ())), preferred_element_type=F32)
        live = at < len_ref[b]
        top = jnp.max(jnp.where(live, s, FLOOR), axis=1, keepdims=True)
        weights = jnp.where(live, jnp.exp(s - top), 0.0)
        total = jnp.sum(weights, axis=1, keepdims=True)
        out_ref[b, :heads, :] = jnp.dot(
            weights.astype(BF16), v_ref[b], preferred_element_type=F32
        )
        tops = jnp.where(lane == b, top, tops)
        totals = jnp.where(lane == b, total, totals)
    spare = jnp.zeros((HD - 2 * heads, HD), F32)
    turned = jnp.concatenate([tops, totals, spare], axis=0).T
    out_ref[:, heads, :] = turned[:rows]


def combine(got_ref, mine_ref, knew_ref, vnew_ref, all_ref):
    n, _, _ = got_ref.shape
    heads = mine_ref.shape[0]
    me = lax.axis_index("seq")
    chosen = lax.broadcasted_iota(jnp.int32, (knew_ref.shape[0], HD), 0) == me
    k_row = jnp.sum(jnp.where(chosen, knew_ref[...].astype(F32), 0.0), axis=0, keepdims=True)
    v_row = jnp.sum(jnp.where(chosen, vnew_ref[...].astype(F32), 0.0), axis=0, keepdims=True)
    own = jnp.sum(mine_ref[...] * k_row, axis=1, keepdims=True)
    stats = got_ref[:, heads, :]
    stats = jnp.concatenate([stats, jnp.zeros((HD - n, HD), F32)], axis=0).T
    tops = stats[:heads]
    totals = stats[heads : 2 * heads]
    lane = lax.broadcasted_iota(jnp.int32, (heads, HD), 1)
    tops = jnp.where(lane < n, tops, FLOOR)
    top = jnp.maximum(jnp.max(tops, axis=1, keepdims=True), own)
    factor = jnp.exp(tops - top)
    fresh = jnp.exp(own - top)
    total = jnp.sum(factor * totals, axis=1, keepdims=True) + fresh
    summed = fresh * v_row
    for i in range(n):
        summed = summed + factor[:, i : i + 1] * got_ref[i, :heads, :]
    result = (summed / total).astype(BF16).astype(F32)
    for i in range(n):
        all_ref[i] = result


def project_out(a_ref, w_ref, kept_ref, given_ref):
    _, heads, _ = a_ref.shape
    lines = jnp.concatenate([a_ref[:, h, :] for h in range(heads)], axis=1).astype(BF16)
    out = jnp.dot(lines, w_ref[...], preferred_element_type=F32)
    half = out.shape[1] // 2
    first = lax.axis_index("head") == 0
    left, right = out[:, :half], out[:, half:]
    kept_ref[...] = jnp.where(first, left, right)
    given_ref[...] = jnp.where(first, right, left)


def shards(
    hidden_in,
    norm_gain_vector,
    w_query,
    key_cache_rows,
    value_cache_rows,
    k_new,
    v_new,
    lengths,
    w_out,
):
    rows, width = hidden_in.shape
    heads = w_query.shape[1] // HD
    n = lax.axis_size("seq")
    assert rows == n and 2 * heads <= HD
    tall = (n, heads + 8, HD)
    flat = (n, heads, HD)
    (sent,) = call(project, [tall], hidden_in, norm_gain_vector.reshape(1, -1), w_query)
    got = exchanged(sent, "seq")
    sent, mine = call(functools.partial(finish_query, width * n), [flat, flat[1:]], got)
    queries = exchanged(sent, "seq")
    (sent,) = call(
        attend, [tall], queries, key_cache_rows, value_cache_rows, lengths, smem=(3,), mib=24
    )
    got = exchanged(sent, "seq")
    (sent,) = call(combine, [flat], got, mine, k_new, v_new)
    attended = exchanged(sent, "seq")
    half = (rows, w_out.shape[1] // 2)
    kept, given = call(project_out, [half, half], attended, w_out)
    return kept + swapped(given, "head")


def solution(mesh):
    placed = (
        P(("groups", "batch"), "seq"),
        P("seq"),
        P("seq", "head"),
        P(("groups", "batch"), "seq", None),
        P(("groups", "batch"), "seq", None),
        P(("groups", "batch"), None),
        P(("groups", "batch"), None),
        P(("groups", "batch")),
        P("head", "seq"),
    )
    return jax.shard_map(
        shards,
        mesh=mesh,
        in_specs=placed,
        out_specs=P(("groups", "batch"), ("seq", "head")),
        check_vma=False,
    )
```

```python
import functools

import jax
import jax.numpy as jnp
from jax import lax
from jax.experimental import pallas as pl
from jax.experimental.pallas import tpu as pltpu
from jax.sharding import PartitionSpec as P

HD = 128
FLOOR = -1e30
F32 = jnp.float32
BF16 = jnp.bfloat16


def exchanged(blocks, axis):
    return lax.all_to_all(blocks, axis, split_axis=0, concat_axis=0, tiled=True)


def parts_exchanged(lines):
    return exchanged(lines.reshape(-1, 1, HD), "seq").reshape(lines.shape)


def swapped(array, axis):
    return lax.ppermute(array, axis, [(0, 1), (1, 0)])


def call(kernel, shapes, *args, away=(), scratch=(), mib=16):
    spaces = [pltpu.HBM if i in away else pltpu.VMEM for i in range(len(args))]
    args = [
        pltpu.with_memory_space_constraint(a, pltpu.HBM) if i in away else a
        for i, a in enumerate(args)
    ]
    return pl.pallas_call(
        kernel,
        out_shape=[jax.ShapeDtypeStruct(s, F32) for s in shapes],
        in_specs=[pl.BlockSpec(memory_space=s) for s in spaces],
        out_specs=[pl.BlockSpec(memory_space=pltpu.VMEM) for _ in shapes],
        scratch_shapes=scratch,
        compiler_params=pltpu.CompilerParams(vmem_limit_bytes=mib << 20),
    )(*args)


def project(x_hbm, g_hbm, w_hbm, out_ref, x_ref, g_ref, w_ref, sems):
    pairs = ((x_hbm, x_ref), (g_hbm, g_ref), (w_hbm, w_ref))
    copies = [pltpu.make_async_copy(a, b, sems.at[i]) for i, (a, b) in enumerate(pairs)]
    for copy in copies:
        copy.start()
    copies[0].wait()
    copies[1].wait()
    rows, width = x_ref.shape
    x = x_ref[...].astype(F32)
    squares = jnp.sum(x * x, axis=1, keepdims=True)
    scaled = x * g_ref[...].astype(F32).reshape(1, width)
    high = scaled.astype(BF16)
    low = (scaled - high.astype(F32)).astype(BF16)
    both = jnp.concatenate([high, low], axis=0)
    copies[2].wait()
    part = jnp.dot(both, w_ref[...], preferred_element_type=F32)
    part = part[:rows] + part[rows:]
    heads = part.shape[1] // HD
    squares = jnp.broadcast_to(squares, (rows, HD))
    for b in range(rows):
        lines = [part[b : b + 1, h * HD : (h + 1) * HD] for h in range(heads)]
        out_ref[b * (heads + 1) : (b + 1) * (heads + 1), :] = jnp.concatenate(
            [*lines, squares[b : b + 1]], axis=0
        )


def finish_query(features, got_ref, all_ref, mine_ref):
    heads = mine_ref.shape[0]
    tall = heads + 1
    n = got_ref.shape[0] // tall
    total = got_ref[:tall, :]
    for i in range(1, n):
        total = total + got_ref[i * tall : (i + 1) * tall, :]
    scale = lax.rsqrt(total[heads:tall] / features + 1e-05)
    root = 1.0 / HD**0.5
    mine = (total[:heads] * scale * root).astype(BF16).astype(F32)
    mine_ref[...] = mine
    for i in range(n):
        all_ref[i] = mine


def attend(q_ref, k_hbm, v_hbm, len_hbm, out_ref, k_ref, v_ref, len_ref, sems, len_sem):
    rows, heads, _ = q_ref.shape
    block = k_ref.shape[1]
    chunks = sems.shape[1]
    step = rows // chunks
    used = pltpu.make_async_copy(len_hbm, len_ref, len_sem)
    used.start()
    copies = []
    for c in range(chunks):
        at = pl.ds(c * step, step)
        keys = pltpu.make_async_copy(k_hbm.at[at], k_ref.at[at], sems.at[0, c])
        values = pltpu.make_async_copy(v_hbm.at[at], v_ref.at[at], sems.at[1, c])
        keys.start()
        values.start()
        copies.append((keys, values))
    used.wait()
    start = lax.axis_index("seq") * block
    at = start + lax.broadcasted_iota(jnp.int32, (heads, block), 1)
    lane = lax.broadcasted_iota(jnp.int32, (heads, HD), 1)
    tops = jnp.zeros((heads, HD), F32)
    totals = jnp.zeros((heads, HD), F32)
    tall = heads + 1
    for b in range(rows):
        if b % step == 0:
            copies[b // step][0].wait()
        q = q_ref[b].astype(BF16)
        s = lax.dot_general(q, k_ref[b], (((1,), (1,)), ((), ())), preferred_element_type=F32)
        live = at < len_ref[b]
        top = jnp.max(jnp.where(live, s, FLOOR), axis=1, keepdims=True)
        weights = jnp.where(live, jnp.exp(s - top), 0.0)
        total = jnp.sum(weights, axis=1, keepdims=True)
        if b % step == 0:
            copies[b // step][1].wait()
        out_ref[b * tall : b * tall + heads, :] = jnp.dot(
            weights.astype(BF16), v_ref[b], preferred_element_type=F32
        )
        tops = jnp.where(lane == b, top, tops)
        totals = jnp.where(lane == b, total, totals)
    spare = jnp.zeros((HD - 2 * heads, HD), F32)
    turned = jnp.concatenate([tops, totals, spare], axis=0).T
    for b in range(rows):
        out_ref[b * tall + heads : (b + 1) * tall, :] = turned[b : b + 1]


def combine(got_ref, mine_ref, knew_ref, vnew_ref, all_ref):
    heads = mine_ref.shape[0]
    tall = heads + 1
    n = got_ref.shape[0] // tall
    me = lax.axis_index("seq")
    chosen = lax.broadcasted_iota(jnp.int32, (knew_ref.shape[0], HD), 0) == me
    k_row = jnp.sum(jnp.where(chosen, knew_ref[...].astype(F32), 0.0), axis=0, keepdims=True)
    v_row = jnp.sum(jnp.where(chosen, vnew_ref[...].astype(F32), 0.0), axis=0, keepdims=True)
    own = jnp.sum(mine_ref[...] * k_row, axis=1, keepdims=True)
    stats = [got_ref[i * tall + heads : (i + 1) * tall, :] for i in range(n)]
    stats = jnp.concatenate([*stats, jnp.zeros((HD - n, HD), F32)], axis=0).T
    tops = stats[:heads]
    totals = stats[heads : 2 * heads]
    lane = lax.broadcasted_iota(jnp.int32, (heads, HD), 1)
    tops = jnp.where(lane < n, tops, FLOOR)
    top = jnp.maximum(jnp.max(tops, axis=1, keepdims=True), own)
    factor = jnp.exp(tops - top)
    fresh = jnp.exp(own - top)
    total = jnp.sum(factor * totals, axis=1, keepdims=True) + fresh
    summed = fresh * v_row
    for i in range(n):
        summed = summed + factor[:, i : i + 1] * got_ref[i * tall : i * tall + heads, :]
    result = (summed / total).astype(BF16).astype(F32)
    for i in range(n):
        all_ref[i] = result


def project_out(a_ref, w_ref, kept_ref, given_ref):
    _, heads, _ = a_ref.shape
    lines = jnp.concatenate([a_ref[:, h, :] for h in range(heads)], axis=1).astype(BF16)
    out = jnp.dot(lines, w_ref[...], preferred_element_type=F32)
    half = out.shape[1] // 2
    first = lax.axis_index("head") == 0
    left, right = out[:, :half], out[:, half:]
    kept_ref[...] = jnp.where(first, left, right)
    given_ref[...] = jnp.where(first, right, left)


def shards(
    hidden_in,
    norm_gain_vector,
    w_query,
    key_cache_rows,
    value_cache_rows,
    k_new,
    v_new,
    lengths,
    w_out,
):
    rows, width = hidden_in.shape
    heads = w_query.shape[1] // HD
    n = lax.axis_size("seq")
    assert rows == n and 2 * heads <= HD
    tall = (n * (heads + 1), HD)
    flat = (n, heads, HD)
    dma = pltpu.SemaphoreType.DMA
    (sent,) = call(
        project,
        [tall],
        hidden_in,
        norm_gain_vector,
        w_query,
        away=(0, 1, 2),
        scratch=[
            pltpu.VMEM(hidden_in.shape, BF16),
            pltpu.VMEM(norm_gain_vector.shape, BF16),
            pltpu.VMEM(w_query.shape, BF16),
            dma((3,)),
        ],
    )
    got = parts_exchanged(sent)
    sent, mine = call(functools.partial(finish_query, width * n), [flat, flat[1:]], got)
    queries = exchanged(sent, "seq")
    (sent,) = call(
        attend,
        [tall],
        queries,
        key_cache_rows,
        value_cache_rows,
        lengths,
        away=(1, 2, 3),
        scratch=[
            pltpu.VMEM(key_cache_rows.shape, BF16),
            pltpu.VMEM(value_cache_rows.shape, BF16),
            pltpu.SMEM(lengths.shape, jnp.int32),
            dma((2, rows // 2)),
            dma(()),
        ],
        mib=24,
    )
    got = parts_exchanged(sent)
    (sent,) = call(combine, [flat], got, mine, k_new, v_new)
    attended = exchanged(sent, "seq")
    half = (rows, w_out.shape[1] // 2)
    kept, given = call(project_out, [half, half], attended, w_out)
    return kept + swapped(given, "head")


def solution(mesh):
    placed = (
        P(("groups", "batch"), "seq"),
        P("seq"),
        P("seq", "head"),
        P(("groups", "batch"), "seq", None),
        P(("groups", "batch"), "seq", None),
        P(("groups", "batch"), None),
        P(("groups", "batch"), None),
        P(("groups", "batch")),
        P("head", "seq"),
    )
    return jax.shard_map(
        shards,
        mesh=mesh,
        in_specs=placed,
        out_specs=P(("groups", "batch"), ("seq", "head")),
        check_vma=False,
    )
```

```python
import functools

import jax
import jax.numpy as jnp
from jax import lax
from jax.experimental import pallas as pl
from jax.experimental.pallas import tpu as pltpu
from jax.sharding import PartitionSpec as P


HD = 128
QUAD = 4
FLOOR = -1e30
AHEAD = 20_000_000_000
F32 = jnp.float32
BF16 = jnp.bfloat16


def swapped(array, axis):
    return lax.ppermute(array, axis, [(0, 1), (1, 0)])


def inside(blocks, nearest_first=True):
    n = lax.axis_size("seq")
    got = [
        lax.ppermute(block, "seq", [(i, i ^ k) for i in range(n)])
        for k, block in enumerate(blocks, 1)
    ]
    return got if nearest_first else got[::-1]


def between(block):
    n = lax.axis_size("seq")
    return [
        lax.ppermute(block, "seq", [(i, (i + k) % n) for i in range(n)])
        for k in sorted(range(QUAD, n, QUAD), key=lambda k: min(k, n - k))
    ]


def call(kernel, shapes, *args, away=(), smem=(), scratch=(), mib=8, flops=0):
    def space(i):
        return pltpu.HBM if i in away else pltpu.SMEM if i in smem else pltpu.VMEM

    args = [
        pltpu.with_memory_space_constraint(a, pltpu.HBM) if i in away else a
        for i, a in enumerate(args)
    ]
    return pl.pallas_call(
        kernel,
        out_shape=[jax.ShapeDtypeStruct(s, F32) for s in shapes],
        in_specs=[pl.BlockSpec(memory_space=space(i)) for i in range(len(args))],
        out_specs=[pl.BlockSpec(memory_space=pltpu.VMEM) for _ in shapes],
        scratch_shapes=scratch,
        compiler_params=pltpu.CompilerParams(vmem_limit_bytes=mib << 20),
        cost_estimate=pl.CostEstimate(flops=flops, transcendentals=0, bytes_accessed=0)
        if flops
        else None,
    )(*args)


def place():
    return lax.rem(lax.axis_index("seq"), QUAD)


def hand_out(chunk_ref, out_refs):
    mine = place()
    for k, out_ref in enumerate(out_refs):
        out_ref[...] = chunk_ref[mine ^ k]


def lay_out(got_refs, all_ref):
    mine = place()
    share = got_refs[0].shape[0]
    for k, got_ref in enumerate(got_refs):
        all_ref[pl.ds((mine ^ k) * share, share)] = got_ref[...]


def project(x_hbm, g_hbm, w_hbm, *refs):
    *out_refs, x_ref, g_ref, w_ref, chunk_ref, sems = refs
    pairs = ((x_hbm, x_ref), (g_hbm, g_ref), (w_hbm, w_ref))
    copies = [pltpu.make_async_copy(a, b, sems.at[i]) for i, (a, b) in enumerate(pairs)]
    for copy in copies:
        copy.start()
    copies[0].wait()
    copies[1].wait()
    rows, width = x_ref.shape
    x = x_ref[...].astype(F32)
    squares = jnp.sum(x * x, axis=1, keepdims=True)
    scaled = x * g_ref[...].astype(F32).reshape(1, width)
    high = scaled.astype(BF16)
    low = (scaled - high.astype(F32)).astype(BF16)
    both = jnp.concatenate([high, low], axis=0)
    copies[2].wait()
    part = jnp.dot(both, w_ref[...], preferred_element_type=F32)
    part = part[:rows] + part[rows:]
    heads = part.shape[1] // HD
    squares = jnp.broadcast_to(squares, (rows, HD))
    share = rows // QUAD
    for b in range(rows):
        c, i = b // share, b % share
        lines = [part[b : b + 1, h * HD : (h + 1) * HD] for h in range(heads)]
        chunk_ref[c, i * heads : (i + 1) * heads, :] = jnp.concatenate(lines, axis=0)
    for c in range(QUAD):
        mine = squares[c * share : (c + 1) * share]
        chunk_ref[c, share * heads :, :] = jnp.concatenate([mine, mine], axis=0)
    hand_out(chunk_ref, out_refs)


def add_up(*refs):
    *got_refs, out_ref = refs
    out_ref[...] = functools.reduce(jnp.add, [r[...] for r in got_refs])


def finish_query(features, *refs):
    *got_refs, out_ref = refs
    total = functools.reduce(jnp.add, [r[...] for r in got_refs])
    share, heads, _ = out_ref.shape
    scale = lax.rsqrt(total[share * heads :] / features + 1e-05) * (1.0 / HD**0.5)
    for i in range(share):
        mine = total[i * heads : (i + 1) * heads] * scale[i : i + 1]
        out_ref[i] = mine.astype(BF16).astype(F32)


def attend(*refs):
    q_refs, (k_ref, v_ref, len_ref) = refs[:QUAD], refs[QUAD : QUAD + 3]
    *out_refs, q_ref, s_ref, top_ref, chunk_ref = refs[QUAD + 3 :]
    lay_out(q_refs, q_ref)
    rows, heads, _ = q_ref.shape
    share = rows // QUAD
    block = k_ref.shape[1]
    at = lax.axis_index("seq") * block + lax.broadcasted_iota(jnp.int32, (heads, block), 1)
    lane = lax.broadcasted_iota(jnp.int32, (heads, HD), 1)
    tops = jnp.zeros((heads, HD), F32)
    totals = jnp.zeros((heads, HD), F32)
    for b in range(rows):
        q = q_ref[b].astype(BF16)
        s = lax.dot_general(q, k_ref[b], (((1,), (1,)), ((), ())), preferred_element_type=F32)
        s = jnp.where(at < len_ref[b], s, FLOOR)
        s_ref[b] = s
        top = jnp.maximum(jnp.max(s, axis=1, keepdims=True), FLOOR / 2)
        top_ref[b] = jnp.broadcast_to(top, (heads, HD))
        tops = jnp.where(lane == b, top, tops)
    for b in range(rows):
        top = top_ref[b]
        weights = [jnp.exp(s_ref[b, :, i : i + HD] - top) for i in range(0, block, HD)]
        total = jnp.sum(functools.reduce(jnp.add, weights), axis=1, keepdims=True)
        totals = jnp.where(lane == b, total, totals)
        weights = jnp.concatenate([w.astype(BF16) for w in weights], axis=1)
        c, i = b // share, b % share
        chunk_ref[c, i * heads : (i + 1) * heads, :] = jnp.dot(
            weights, v_ref[b], preferred_element_type=F32
        )
    spare = jnp.zeros((HD - heads, HD), F32)
    tops = jnp.concatenate([tops, spare], axis=0).T
    totals = jnp.concatenate([totals, spare], axis=0).T
    for c in range(QUAD):
        mine = slice(c * share, (c + 1) * share)
        chunk_ref[c, share * heads :, :] = jnp.concatenate([tops[mine], totals[mine]], axis=0)
    hand_out(chunk_ref, out_refs)


def joined(got_refs, share, heads):
    at = share * heads
    tops = [r[at : at + share, :] for r in got_refs]
    top = functools.reduce(jnp.maximum, tops)
    factors = [jnp.exp(t - top) for t in tops]
    total = functools.reduce(
        jnp.add, [f * r[at + share :, :] for f, r in zip(factors, got_refs, strict=True)]
    )
    known = len(got_refs) * share + 2 * share
    spare = jnp.zeros((HD - known, HD), F32)
    turned = jnp.concatenate([*factors, top, total, spare], axis=0).T[:heads]
    sums = []
    for i in range(share):
        parts = [
            turned[:, s * share + i : s * share + i + 1] * r[i * heads : (i + 1) * heads, :]
            for s, r in enumerate(got_refs)
        ]
        sums.append(functools.reduce(jnp.add, parts))
    return sums, top, total, turned


def combine(share, heads, *refs):
    *got_refs, out_ref = refs
    sums, top, total, _ = joined(got_refs, share, heads)
    for i in range(share):
        out_ref[i * heads : (i + 1) * heads, :] = sums[i]
    out_ref[share * heads :, :] = jnp.concatenate([top, total], axis=0)


def finish_attention(*refs):
    *got_refs, q_ref, knew_ref, vnew_ref, out_ref = refs
    share, heads, _ = out_ref.shape
    sums, _, _, turned = joined(got_refs, share, heads)
    known = len(got_refs) * share
    keys, values = knew_ref[...].astype(F32), vnew_ref[...].astype(F32)
    row = lax.broadcasted_iota(jnp.int32, keys.shape, 0)
    for i in range(share):
        chosen = row == place() * share + i
        k_row = jnp.sum(jnp.where(chosen, keys, 0.0), axis=0, keepdims=True)
        v_row = jnp.sum(jnp.where(chosen, values, 0.0), axis=0, keepdims=True)
        own = jnp.sum(q_ref[i] * k_row, axis=1, keepdims=True)
        old = turned[:, known + i : known + i + 1]
        top = jnp.maximum(old, own)
        factor = jnp.exp(old - top)
        fresh = jnp.exp(own - top)
        total = factor * turned[:, known + share + i : known + share + i + 1] + fresh
        result = (factor * sums[i] + fresh * v_row) / total
        out_ref[i] = result.astype(BF16).astype(F32)


def project_out(*refs):
    *got_refs, w_ref, kept_ref, given_ref, a_ref = refs
    lay_out(got_refs, a_ref)
    heads = a_ref.shape[1]
    lines = jnp.concatenate([a_ref[:, h, :] for h in range(heads)], axis=1).astype(BF16)
    out = jnp.dot(lines, w_ref[...], preferred_element_type=F32)
    half = out.shape[1] // 2
    first = lax.axis_index("head") == 0
    left, right = out[:, :half], out[:, half:]
    kept_ref[...] = jnp.where(first, left, right)
    given_ref[...] = jnp.where(first, right, left)


def shards(
    hidden_in,
    norm_gain_vector,
    w_query,
    key_cache_rows,
    value_cache_rows,
    k_new,
    v_new,
    lengths,
    w_out,
):
    rows, width = hidden_in.shape
    heads = w_query.shape[1] // HD
    n = lax.axis_size("seq")
    block = key_cache_rows.shape[1]
    share = rows // QUAD
    assert n % QUAD == 0 and share * QUAD == rows and 2 * share == 8
    chunk = (share * heads + 2 * share, HD)
    held = (share, heads, HD)
    whole = (rows, heads, HD)
    chunks = pltpu.VMEM((QUAD, *chunk), F32)
    mine, *sent = call(
        project,
        [chunk] * QUAD,
        hidden_in,
        norm_gain_vector,
        w_query,
        away=(0, 1, 2),
        scratch=[
            pltpu.VMEM(hidden_in.shape, BF16),
            pltpu.VMEM(norm_gain_vector.shape, BF16),
            pltpu.VMEM(w_query.shape, BF16),
            chunks,
            pltpu.SemaphoreType.DMA((3,)),
        ],
    )
    (mine,) = call(add_up, [chunk], mine, *inside(sent, False), flops=AHEAD)
    finish = functools.partial(finish_query, width * n)
    (queries,) = call(finish, [held], mine, *between(mine))
    mine, *sent = call(
        attend,
        [chunk] * QUAD,
        queries,
        *inside([queries] * 3),
        key_cache_rows,
        value_cache_rows,
        lengths,
        smem=(QUAD + 2,),
        scratch=[
            pltpu.VMEM(whole, F32),
            pltpu.VMEM((rows, heads, block), F32),
            pltpu.VMEM(whole, F32),
            chunks,
        ],
    )
    (mine,) = call(functools.partial(combine, share, heads), [chunk], mine, *inside(sent, False))
    (attended,) = call(finish_attention, [held], mine, *between(mine), queries, k_new, v_new)
    half = (rows, w_out.shape[1] // 2)
    kept, given = call(
        project_out,
        [half, half],
        attended,
        *inside([attended] * 3),
        w_out,
        scratch=[pltpu.VMEM(whole, F32)],
    )
    return kept + swapped(given, "head")


def solution(mesh):
    placed = (
        P(("groups", "batch"), "seq"),
        P("seq"),
        P("seq", "head"),
        P(("groups", "batch"), "seq", None),
        P(("groups", "batch"), "seq", None),
        P(("groups", "batch"), None),
        P(("groups", "batch"), None),
        P(("groups", "batch")),
        P("head", "seq"),
    )
    return jax.shard_map(
        shards,
        mesh=mesh,
        in_specs=placed,
        out_specs=P(("groups", "batch"), ("seq", "head")),
        check_vma=False,
    )
```

```python
import functools

import jax
import jax.numpy as jnp
from jax import lax
from jax.experimental import pallas as pl
from jax.experimental.pallas import tpu as pltpu
from jax.sharding import PartitionSpec as P


HD = 128
QUAD = 4
APART = (3, 2, 1)
FLOOR = -1e30
AHEAD = 20_000_000_000
F32 = jnp.float32
BF16 = jnp.bfloat16


def swapped(array):
    return lax.ppermute(array, "head", [(0, 1), (1, 0)])


def passed(block, targets):
    n, wide, cores = (lax.axis_size(a) for a in ("seq", "batch", "head"))
    pairs = []
    for i in range(n):
        for x in range(wide):
            for core, target in enumerate(targets):
                z, w = (i, x ^ 1) if target is None else (target(i) % n, x)
                pairs.append(((i * wide + x) * cores + core, (z * wide + w) * cores + core))
    return lax.ppermute(block, ("seq", "batch", "head"), pairs)


def inside(first, second):
    return [
        passed(first, (lambda i: i ^ 2, lambda i: i ^ 3)),
        passed(second, (None, lambda i: i ^ 1)),
    ]


def scattered(blocks):
    n = lax.axis_size("seq")
    return [
        lax.ppermute(block, "seq", [(i, i ^ k) for i in range(n)])
        for k, block in zip(APART, blocks, strict=True)
    ]


def between(block):
    n = lax.axis_size("seq")
    return [
        passed(block, (lambda i: i + QUAD, lambda i: i + n // 2)),
        passed(block, (lambda i: i - QUAD, None)),
    ]


def call(kernel, shapes, *args, away=(), smem=(), scratch=(), mib=8, flops=0):
    def space(i):
        return pltpu.HBM if i in away else pltpu.SMEM if i in smem else pltpu.VMEM

    args = [
        pltpu.with_memory_space_constraint(a, pltpu.HBM) if i in away else a
        for i, a in enumerate(args)
    ]
    return pl.pallas_call(
        kernel,
        out_shape=[jax.ShapeDtypeStruct(s, F32) for s in shapes],
        in_specs=[pl.BlockSpec(memory_space=space(i)) for i in range(len(args))],
        out_specs=[pl.BlockSpec(memory_space=pltpu.VMEM) for _ in shapes],
        scratch_shapes=scratch,
        compiler_params=pltpu.CompilerParams(vmem_limit_bytes=mib << 20),
        cost_estimate=pl.CostEstimate(flops=flops, transcendentals=0, bytes_accessed=0)
        if flops
        else None,
    )(*args)


def core():
    return lax.axis_index("head")


def chosen():
    mine = lax.rem(lax.axis_index("seq"), QUAD)
    return mine ^ (2 + core()), mine ^ core()


def either(a_ref, b_ref):
    return jnp.where(core() == 1, b_ref[...], a_ref[...])


def project(x_hbm, g_hbm, w_hbm, *refs):
    *out_refs, x_ref, g_ref, w_ref, chunk_ref, sems = refs
    pairs = ((x_hbm, x_ref), (g_hbm, g_ref), (w_hbm, w_ref))
    copies = [pltpu.make_async_copy(a, b, sems.at[i]) for i, (a, b) in enumerate(pairs)]
    for copy in copies:
        copy.start()
    copies[0].wait()
    copies[1].wait()
    rows, width = x_ref.shape
    x = x_ref[...].astype(F32)
    squares = jnp.sum(x * x, axis=1, keepdims=True)
    scaled = x * g_ref[...].astype(F32).reshape(1, width)
    high = scaled.astype(BF16)
    low = (scaled - high.astype(F32)).astype(BF16)
    both = jnp.concatenate([high, low], axis=0)
    copies[2].wait()
    part = jnp.dot(both, w_ref[...], preferred_element_type=F32)
    part = part[:rows] + part[rows:]
    heads = part.shape[1] // HD
    squares = jnp.broadcast_to(squares, (rows, HD))
    share = rows // QUAD
    for b in range(rows):
        c, i = b // share, b % share
        lines = [part[b : b + 1, h * HD : (h + 1) * HD] for h in range(heads)]
        chunk_ref[c, i * heads : (i + 1) * heads, :] = jnp.concatenate(lines, axis=0)
    for c in range(QUAD):
        mine = squares[c * share : (c + 1) * share]
        chunk_ref[c, share * heads :, :] = jnp.concatenate([mine, mine], axis=0)
    place = lax.rem(lax.axis_index("seq"), QUAD)
    for k, out_ref in zip((0, *APART), out_refs, strict=True):
        out_ref[...] = chunk_ref[place ^ k]


def widen(w_ref, after_ref, out_ref):
    out_ref[...] = w_ref[...].astype(F32)


def rotated(kernel):
    def turned(a_ref, b_ref, first_ref, *refs):
        kernel(first_ref, a_ref, b_ref, *refs)

    return turned


def add_up(*refs):
    *got_refs, out_ref = refs
    out_ref[...] = functools.reduce(jnp.add, [r[...] for r in got_refs])


def both_cores(share, own_ref, other_ref, out_ref):
    half = (own_ref.shape[0] - 2 * share) // share
    own, other = own_ref[...], other_ref[...]
    low = jnp.where(core() == 0, own, other)
    high = jnp.where(core() == 0, other, own)
    for i in range(share):
        at = slice(i * half, (i + 1) * half)
        out_ref[2 * i * half : 2 * (i + 1) * half, :] = jnp.concatenate([low[at], high[at]], axis=0)
    out_ref[2 * share * half :, :] = own[share * half :]


def add_either(got_ref, a_ref, b_ref, out_ref):
    out_ref[...] = got_ref[...] + either(a_ref, b_ref)


def finish_query(features, a_ref, b_ref, out_ref):
    total = a_ref[...] + b_ref[...]
    share, heads, _ = out_ref.shape
    scale = lax.rsqrt(total[share * heads :] / features + 1e-05) * (1.0 / HD**0.5)
    for i in range(share):
        mine = total[i * heads : (i + 1) * heads] * scale[i : i + 1]
        out_ref[i] = mine.astype(BF16).astype(F32)


def attend(first_ref, a_ref, b_ref, k_ref, v_ref, len_ref, *refs):
    *out_refs, q_ref, s_ref, top_ref = refs
    share, heads, _ = first_ref.shape
    q_ref[:share] = first_ref[...]
    q_ref[share:] = either(a_ref, b_ref)
    block = k_ref.shape[1]
    at = lax.axis_index("seq") * block + lax.broadcasted_iota(jnp.int32, (heads, block), 1)
    lane = lax.broadcasted_iota(jnp.int32, (heads, HD), 1)
    tops = jnp.zeros((heads, HD), F32)
    totals = jnp.zeros((heads, HD), F32)
    rows = [place * share + i for place in chosen() for i in range(share)]
    for j, b in enumerate(rows):
        q = q_ref[j].astype(BF16)
        s = lax.dot_general(q, k_ref[b], (((1,), (1,)), ((), ())), preferred_element_type=F32)
        s = jnp.where(at < len_ref[b], s, FLOOR)
        s_ref[j] = s
        top = jnp.maximum(jnp.max(s, axis=1, keepdims=True), FLOOR / 2)
        top_ref[j] = jnp.broadcast_to(top, (heads, HD))
        tops = jnp.where(lane == j, top, tops)
    for j, b in enumerate(rows):
        top = top_ref[j]
        weights = [jnp.exp(s_ref[j, :, i : i + HD] - top) for i in range(0, block, HD)]
        total = jnp.sum(functools.reduce(jnp.add, weights), axis=1, keepdims=True)
        totals = jnp.where(lane == j, total, totals)
        weights = jnp.concatenate([w.astype(BF16) for w in weights], axis=1)
        out_ref, i = out_refs[j // share], j % share
        out_ref[i * heads : (i + 1) * heads, :] = jnp.dot(
            weights, v_ref[b], preferred_element_type=F32
        )
    spare = jnp.zeros((HD - heads, HD), F32)
    tops = jnp.concatenate([tops, spare], axis=0).T
    totals = jnp.concatenate([totals, spare], axis=0).T
    for c, out_ref in enumerate(out_refs):
        mine = slice(c * share, (c + 1) * share)
        out_ref[share * heads :, :] = jnp.concatenate([tops[mine], totals[mine]], axis=0)


def joined(blocks, share, heads):
    at = share * heads
    tops = [r[at : at + share] for r in blocks]
    top = functools.reduce(jnp.maximum, tops)
    factors = [jnp.exp(t - top) for t in tops]
    total = functools.reduce(
        jnp.add, [f * r[at + share :] for f, r in zip(factors, blocks, strict=True)]
    )
    known = len(blocks) * share + 2 * share
    spare = jnp.zeros((HD - known, HD), F32)
    turned = jnp.concatenate([*factors, top, total, spare], axis=0).T[:heads]
    sums = []
    for i in range(share):
        parts = [
            turned[:, s * share + i : s * share + i + 1] * r[i * heads : (i + 1) * heads]
            for s, r in enumerate(blocks)
        ]
        sums.append(functools.reduce(jnp.add, parts))
    return sums, top, total, turned


def join(blocks, share, heads, out_ref):
    sums, top, total, _ = joined(blocks, share, heads)
    for i in range(share):
        out_ref[i * heads : (i + 1) * heads, :] = sums[i]
    out_ref[share * heads :, :] = jnp.concatenate([top, total], axis=0)


def join_pair(share, heads, a_ref, b_ref, out_ref):
    join([a_ref[...], b_ref[...]], share, heads, out_ref)


def join_either(share, heads, got_ref, a_ref, b_ref, out_ref):
    join([got_ref[...], either(a_ref, b_ref)], share, heads, out_ref)


def finish_attention(a_ref, b_ref, q_ref, knew_ref, vnew_ref, out_ref):
    share, heads, _ = out_ref.shape
    sums, _, _, turned = joined([a_ref[...], b_ref[...]], share, heads)
    known = 2 * share
    keys, values = knew_ref[...].astype(F32), vnew_ref[...].astype(F32)
    row = lax.broadcasted_iota(jnp.int32, keys.shape, 0)
    first = lax.rem(lax.axis_index("seq"), QUAD) * share
    for i in range(share):
        k_row = jnp.sum(jnp.where(row == first + i, keys, 0.0), axis=0, keepdims=True)
        v_row = jnp.sum(jnp.where(row == first + i, values, 0.0), axis=0, keepdims=True)
        own = jnp.sum(q_ref[i] * k_row, axis=1, keepdims=True)
        old = turned[:, known + i : known + i + 1]
        top = jnp.maximum(old, own)
        factor = jnp.exp(old - top)
        fresh = jnp.exp(own - top)
        total = factor * turned[:, known + share + i : known + share + i + 1] + fresh
        result = (factor * sums[i] + fresh * v_row) / total
        out_ref[i] = result.astype(BF16).astype(F32)


def project_out(first_ref, a_ref, b_ref, own_ref, other_ref, kept_ref, given_ref, all_ref):
    share, heads, _ = first_ref.shape
    all_ref[:share] = first_ref[...]
    all_ref[share:] = either(a_ref, b_ref)
    half = heads // 2
    zeroth = core() == 0
    low = jnp.concatenate([all_ref[:, h, :] for h in range(half)], axis=1)
    high = jnp.concatenate([all_ref[:, half + h, :] for h in range(half)], axis=1)
    own = jnp.where(zeroth, low, high).astype(BF16)
    other = jnp.where(zeroth, high, low).astype(BF16)
    out = jnp.dot(own, own_ref[...], preferred_element_type=F32)
    out += jnp.dot(other, other_ref[...].astype(BF16), preferred_element_type=F32)
    width = out.shape[1] // 2
    left, right = out[:, :width], out[:, width:]
    kept_ref[...] = jnp.where(zeroth, left, right)
    given_ref[...] = jnp.where(zeroth, right, left)


def put_in_order(kept_ref, got_ref, out_ref):
    share = kept_ref.shape[0] // 2
    far, near = chosen()
    kept, got = kept_ref[...], got_ref[...]
    for c in range(QUAD):
        mine = jnp.where(far == c, kept[:share], kept[share:])
        given = jnp.where((far ^ 1) == c, got[:share], got[share:])
        here = (far == c) | (near == c)
        out_ref[c * share : (c + 1) * share, :] = jnp.where(here, mine, given)


def shards(
    hidden_in,
    norm_gain_vector,
    w_query,
    key_cache_rows,
    value_cache_rows,
    k_new,
    v_new,
    lengths,
    w_out,
):
    rows, width = hidden_in.shape
    half = w_query.shape[1] // HD
    heads = 2 * half
    n = lax.axis_size("seq")
    block = key_cache_rows.shape[1]
    share = rows // QUAD
    assert n == QUAD * QUAD and share * QUAD == rows and 2 * share == 8
    assert lax.axis_size("head") == 2 and lax.axis_size("batch") % 2 == 0 and heads <= HD
    chunk = (share * heads + 2 * share, HD)
    held = (share, heads, HD)
    twice = (2 * share, heads, HD)
    sizes = (share, heads)
    part = (share * half + 2 * share, HD)
    mine, *sent = call(
        project,
        [part] * QUAD,
        hidden_in,
        norm_gain_vector,
        w_query,
        away=(0, 1, 2),
        scratch=[
            pltpu.VMEM(hidden_in.shape, BF16),
            pltpu.VMEM(norm_gain_vector.shape, BF16),
            pltpu.VMEM(w_query.shape, BF16),
            pltpu.VMEM((QUAD, *part), F32),
            pltpu.SemaphoreType.DMA((3,)),
        ],
    )
    (wide,) = call(widen, [w_out.shape], w_out, mine)
    w_other = swapped(wide)
    (mine,) = call(add_up, [part], mine, *scattered(sent), flops=AHEAD)
    (mine,) = call(functools.partial(both_cores, share), [chunk], mine, swapped(mine))
    got, near = between(mine)
    (mine,) = call(rotated(add_either), [chunk], near, mine, got)
    finish = functools.partial(finish_query, width * n)
    (queries,) = call(finish, [held], mine, swapped(mine))
    got, near = inside(queries, queries)
    first, second = call(
        rotated(attend),
        [chunk] * 2,
        queries,
        near,
        got,
        key_cache_rows,
        value_cache_rows,
        lengths,
        smem=(5,),
        scratch=[
            pltpu.VMEM(twice, F32),
            pltpu.VMEM((2 * share, heads, block), F32),
            pltpu.VMEM(twice, F32),
        ],
    )
    got, near = inside(first, second)
    (mine,) = call(functools.partial(join_either, *sizes), [chunk], got, second, near)
    (mine,) = call(functools.partial(join_pair, *sizes), [chunk], mine, swapped(mine))
    got, near = between(mine)
    (mine,) = call(rotated(functools.partial(join_either, *sizes)), [chunk], near, mine, got)
    (attended,) = call(
        finish_attention, [held], mine, swapped(mine), queries, k_new, v_new
    )
    got, near = inside(attended, attended)
    kept, given = call(
        rotated(project_out),
        [(2 * share, w_out.shape[1] // 2)] * 2,
        attended,
        near,
        got,
        w_out,
        w_other,
        scratch=[pltpu.VMEM(twice, F32)],
    )
    (out,) = call(put_in_order, [(rows, w_out.shape[1] // 2)], kept, swapped(given))
    return out


def solution(mesh):
    placed = (
        P(("groups", "batch"), "seq"),
        P("seq"),
        P("seq", "head"),
        P(("groups", "batch"), "seq", None),
        P(("groups", "batch"), "seq", None),
        P(("groups", "batch"), None),
        P(("groups", "batch"), None),
        P(("groups", "batch")),
        P("head", "seq"),
    )
    return jax.shard_map(
        shards,
        mesh=mesh,
        in_specs=placed,
        out_specs=P(("groups", "batch"), ("seq", "head")),
        check_vma=False,
    )
```

```python
import functools

import jax
import jax.numpy as jnp
from jax import lax
from jax.experimental import pallas as pl
from jax.experimental.pallas import tpu as pltpu
from jax.sharding import PartitionSpec as P


HD = 128
QUAD = 4
FLOOR = -1e30
AHEAD = 20_000_000_000
F32 = jnp.float32
BF16 = jnp.bfloat16


def swapped(array):
    return lax.ppermute(array, "head", [(0, 1), (1, 0)])


def passed(block, targets):
    n, wide, cores = (lax.axis_size(a) for a in ("seq", "batch", "head"))
    pairs = []
    for i in range(n):
        for x in range(wide):
            for core, target in enumerate(targets):
                z, w = (i, x ^ 1) if target is None else (target(i) % n, x)
                pairs.append(((i * wide + x) * cores + core, (z * wide + w) * cores + core))
    return lax.ppermute(block, ("seq", "batch", "head"), pairs)


def inside(first, second):
    return [
        passed(first, (lambda i: i ^ 2, lambda i: i ^ 3)),
        passed(second, (None, lambda i: i ^ 1)),
    ]


def between(block):
    n = lax.axis_size("seq")
    return [
        passed(block, (lambda i: i + QUAD, lambda i: i + n // 2)),
        passed(block, (lambda i: i - QUAD, None)),
    ]


def call(kernel, shapes, *args, away=(), smem=(), scratch=(), mib=8, flops=0):
    def space(i):
        return pltpu.HBM if i in away else pltpu.SMEM if i in smem else pltpu.VMEM

    args = [
        pltpu.with_memory_space_constraint(a, pltpu.HBM) if i in away else a
        for i, a in enumerate(args)
    ]
    return pl.pallas_call(
        kernel,
        out_shape=[jax.ShapeDtypeStruct(s, F32) for s in shapes],
        in_specs=[pl.BlockSpec(memory_space=space(i)) for i in range(len(args))],
        out_specs=[pl.BlockSpec(memory_space=pltpu.VMEM) for _ in shapes],
        scratch_shapes=scratch,
        compiler_params=pltpu.CompilerParams(vmem_limit_bytes=mib << 20),
        cost_estimate=pl.CostEstimate(flops=flops, transcendentals=0, bytes_accessed=0)
        if flops
        else None,
    )(*args)


def core():
    return lax.axis_index("head")


def chosen():
    mine = lax.rem(lax.axis_index("seq"), QUAD)
    return mine ^ (2 + core()), mine ^ core()


def either(a_ref, b_ref):
    return jnp.where(core() == 1, b_ref[...], a_ref[...])


def project(x_hbm, g_hbm, w_hbm, part_ref, squares_ref, x_ref, g_ref, w_ref, sems):
    pairs = ((x_hbm, x_ref), (g_hbm, g_ref), (w_hbm, w_ref))
    copies = [pltpu.make_async_copy(a, b, sems.at[i]) for i, (a, b) in enumerate(pairs)]
    for copy in copies:
        copy.start()
    copies[0].wait()
    copies[1].wait()
    rows, width = x_ref.shape
    x = x_ref[...].astype(F32)
    squares = jnp.sum(x * x, axis=1, keepdims=True)
    squares_ref[...] = jnp.broadcast_to(squares, (rows, HD))
    scaled = x * g_ref[...].astype(F32).reshape(1, width)
    high = scaled.astype(BF16)
    low = (scaled - high.astype(F32)).astype(BF16)
    both = jnp.concatenate([high, low], axis=0)
    copies[2].wait()
    part = jnp.dot(both, w_ref[...], preferred_element_type=F32)
    part = part[:rows] + part[rows:]
    for b in range(rows):
        lines = [part[b : b + 1, h * HD : (h + 1) * HD] for h in range(part_ref.shape[1])]
        part_ref[b] = jnp.concatenate(lines, axis=0)


def assemble(own_ref, other_ref, squares_ref, first_ref, second_ref, chunk_ref):
    rows, half, _ = own_ref.shape
    heads = 2 * half
    share = rows // QUAD
    low = jnp.where(core() == 0, own_ref[...], other_ref[...])
    high = jnp.where(core() == 0, other_ref[...], own_ref[...])
    for b in range(rows):
        c, at = b // share, b % share * heads
        chunk_ref[c, at : at + half, :] = low[b]
        chunk_ref[c, at + half : at + heads, :] = high[b]
    squares = squares_ref[...]
    for c in range(QUAD):
        mine = squares[c * share : (c + 1) * share]
        chunk_ref[c, share * heads :, :] = jnp.concatenate([mine, mine], axis=0)
    for place, out_ref in zip(chosen(), (first_ref, second_ref), strict=True):
        out_ref[...] = chunk_ref[place]


def widen(w_ref, after_ref, out_ref):
    out_ref[...] = w_ref[...].astype(F32)


def rotated(kernel):
    def turned(a_ref, b_ref, first_ref, *refs):
        kernel(first_ref, a_ref, b_ref, *refs)

    return turned


def add_pair(a_ref, b_ref, out_ref):
    out_ref[...] = a_ref[...] + b_ref[...]


def add_either(got_ref, a_ref, b_ref, out_ref):
    out_ref[...] = got_ref[...] + either(a_ref, b_ref)


def finish_query(features, a_ref, b_ref, out_ref):
    total = a_ref[...] + b_ref[...]
    share, heads, _ = out_ref.shape
    scale = lax.rsqrt(total[share * heads :] / features + 1e-05) * (1.0 / HD**0.5)
    for i in range(share):
        mine = total[i * heads : (i + 1) * heads] * scale[i : i + 1]
        out_ref[i] = mine.astype(BF16).astype(F32)


def attend(first_ref, a_ref, b_ref, k_ref, v_ref, len_ref, *refs):
    *out_refs, q_ref, s_ref, top_ref = refs
    share, heads, _ = first_ref.shape
    q_ref[:share] = first_ref[...]
    q_ref[share:] = either(a_ref, b_ref)
    block = k_ref.shape[1]
    at = lax.axis_index("seq") * block + lax.broadcasted_iota(jnp.int32, (heads, block), 1)
    lane = lax.broadcasted_iota(jnp.int32, (heads, HD), 1)
    tops = jnp.zeros((heads, HD), F32)
    totals = jnp.zeros((heads, HD), F32)
    rows = [place * share + i for place in chosen() for i in range(share)]
    for j, b in enumerate(rows):
        q = q_ref[j].astype(BF16)
        s = lax.dot_general(q, k_ref[b], (((1,), (1,)), ((), ())), preferred_element_type=F32)
        s = jnp.where(at < len_ref[b], s, FLOOR)
        s_ref[j] = s
        top = jnp.maximum(jnp.max(s, axis=1, keepdims=True), FLOOR / 2)
        top_ref[j] = jnp.broadcast_to(top, (heads, HD))
        tops = jnp.where(lane == j, top, tops)
    for j, b in enumerate(rows):
        top = top_ref[j]
        weights = [jnp.exp(s_ref[j, :, i : i + HD] - top) for i in range(0, block, HD)]
        total = jnp.sum(functools.reduce(jnp.add, weights), axis=1, keepdims=True)
        totals = jnp.where(lane == j, total, totals)
        weights = jnp.concatenate([w.astype(BF16) for w in weights], axis=1)
        out_ref, i = out_refs[j // share], j % share
        out_ref[i * heads : (i + 1) * heads, :] = jnp.dot(
            weights, v_ref[b], preferred_element_type=F32
        )
    spare = jnp.zeros((HD - heads, HD), F32)
    tops = jnp.concatenate([tops, spare], axis=0).T
    totals = jnp.concatenate([totals, spare], axis=0).T
    for c, out_ref in enumerate(out_refs):
        mine = slice(c * share, (c + 1) * share)
        out_ref[share * heads :, :] = jnp.concatenate([tops[mine], totals[mine]], axis=0)


def joined(blocks, share, heads):
    at = share * heads
    tops = [r[at : at + share] for r in blocks]
    top = functools.reduce(jnp.maximum, tops)
    factors = [jnp.exp(t - top) for t in tops]
    total = functools.reduce(
        jnp.add, [f * r[at + share :] for f, r in zip(factors, blocks, strict=True)]
    )
    known = len(blocks) * share + 2 * share
    spare = jnp.zeros((HD - known, HD), F32)
    turned = jnp.concatenate([*factors, top, total, spare], axis=0).T[:heads]
    sums = []
    for i in range(share):
        parts = [
            turned[:, s * share + i : s * share + i + 1] * r[i * heads : (i + 1) * heads]
            for s, r in enumerate(blocks)
        ]
        sums.append(functools.reduce(jnp.add, parts))
    return sums, top, total, turned


def join(blocks, share, heads, out_ref):
    sums, top, total, _ = joined(blocks, share, heads)
    for i in range(share):
        out_ref[i * heads : (i + 1) * heads, :] = sums[i]
    out_ref[share * heads :, :] = jnp.concatenate([top, total], axis=0)


def join_pair(share, heads, a_ref, b_ref, out_ref):
    join([a_ref[...], b_ref[...]], share, heads, out_ref)


def join_either(share, heads, got_ref, a_ref, b_ref, out_ref):
    join([got_ref[...], either(a_ref, b_ref)], share, heads, out_ref)


def finish_attention(a_ref, b_ref, q_ref, knew_ref, vnew_ref, out_ref):
    share, heads, _ = out_ref.shape
    sums, _, _, turned = joined([a_ref[...], b_ref[...]], share, heads)
    known = 2 * share
    keys, values = knew_ref[...].astype(F32), vnew_ref[...].astype(F32)
    row = lax.broadcasted_iota(jnp.int32, keys.shape, 0)
    first = lax.rem(lax.axis_index("seq"), QUAD) * share
    for i in range(share):
        k_row = jnp.sum(jnp.where(row == first + i, keys, 0.0), axis=0, keepdims=True)
        v_row = jnp.sum(jnp.where(row == first + i, values, 0.0), axis=0, keepdims=True)
        own = jnp.sum(q_ref[i] * k_row, axis=1, keepdims=True)
        old = turned[:, known + i : known + i + 1]
        top = jnp.maximum(old, own)
        factor = jnp.exp(old - top)
        fresh = jnp.exp(own - top)
        total = factor * turned[:, known + share + i : known + share + i + 1] + fresh
        result = (factor * sums[i] + fresh * v_row) / total
        out_ref[i] = result.astype(BF16).astype(F32)


def project_out(first_ref, a_ref, b_ref, own_ref, other_ref, kept_ref, given_ref, all_ref):
    share, heads, _ = first_ref.shape
    all_ref[:share] = first_ref[...]
    all_ref[share:] = either(a_ref, b_ref)
    half = heads // 2
    zeroth = core() == 0
    low = jnp.concatenate([all_ref[:, h, :] for h in range(half)], axis=1)
    high = jnp.concatenate([all_ref[:, half + h, :] for h in range(half)], axis=1)
    own = jnp.where(zeroth, low, high).astype(BF16)
    other = jnp.where(zeroth, high, low).astype(BF16)
    out = jnp.dot(own, own_ref[...], preferred_element_type=F32)
    out += jnp.dot(other, other_ref[...].astype(BF16), preferred_element_type=F32)
    width = out.shape[1] // 2
    left, right = out[:, :width], out[:, width:]
    kept_ref[...] = jnp.where(zeroth, left, right)
    given_ref[...] = jnp.where(zeroth, right, left)


def put_in_order(kept_ref, got_ref, out_ref):
    share = kept_ref.shape[0] // 2
    far, near = chosen()
    kept, got = kept_ref[...], got_ref[...]
    lines = []
    for c in range(QUAD):
        mine = jnp.where(far == c, kept[:share], kept[share:])
        given = jnp.where((far ^ 1) == c, got[:share], got[share:])
        here = (far == c) | (near == c)
        lines.append(jnp.where(here, mine, given))
    out_ref[...] = jnp.concatenate(lines, axis=0)


def shards(
    hidden_in,
    norm_gain_vector,
    w_query,
    key_cache_rows,
    value_cache_rows,
    k_new,
    v_new,
    lengths,
    w_out,
):
    rows, width = hidden_in.shape
    half = w_query.shape[1] // HD
    heads = 2 * half
    n = lax.axis_size("seq")
    block = key_cache_rows.shape[1]
    share = rows // QUAD
    assert n == QUAD * QUAD and share * QUAD == rows and 2 * share == 8
    assert lax.axis_size("head") == 2 and lax.axis_size("batch") % 2 == 0 and heads <= HD
    chunk = (share * heads + 2 * share, HD)
    held = (share, heads, HD)
    twice = (2 * share, heads, HD)
    sizes = (share, heads)
    part, squares = call(
        project,
        [(rows, half, HD), (rows, HD)],
        hidden_in,
        norm_gain_vector,
        w_query,
        away=(0, 1, 2),
        scratch=[
            pltpu.VMEM(hidden_in.shape, BF16),
            pltpu.VMEM(norm_gain_vector.shape, BF16),
            pltpu.VMEM(w_query.shape, BF16),
            pltpu.SemaphoreType.DMA((3,)),
        ],
        flops=AHEAD,
    )
    other = swapped(part)
    (wide,) = call(widen, [w_out.shape], w_out, squares)
    w_other = swapped(wide)
    first, second = call(
        assemble,
        [chunk] * 2,
        part,
        other,
        squares,
        scratch=[pltpu.VMEM((QUAD, *chunk), F32)],
    )
    got, near = inside(first, second)
    (mine,) = call(add_either, [chunk], got, second, near, flops=AHEAD)
    (mine,) = call(add_pair, [chunk], mine, swapped(mine))
    got, near = between(mine)
    (mine,) = call(rotated(add_either), [chunk], near, mine, got)
    finish = functools.partial(finish_query, width * n)
    (queries,) = call(finish, [held], mine, swapped(mine))
    got, near = inside(queries, queries)
    first, second = call(
        rotated(attend),
        [chunk] * 2,
        queries,
        near,
        got,
        key_cache_rows,
        value_cache_rows,
        lengths,
        smem=(5,),
        scratch=[
            pltpu.VMEM(twice, F32),
            pltpu.VMEM((2 * share, heads, block), F32),
            pltpu.VMEM(twice, F32),
        ],
    )
    got, near = inside(first, second)
    (mine,) = call(functools.partial(join_either, *sizes), [chunk], got, second, near)
    (mine,) = call(functools.partial(join_pair, *sizes), [chunk], mine, swapped(mine))
    got, near = between(mine)
    (mine,) = call(rotated(functools.partial(join_either, *sizes)), [chunk], near, mine, got)
    (attended,) = call(
        finish_attention, [held], mine, swapped(mine), queries, k_new, v_new
    )
    got, near = inside(attended, attended)
    kept, given = call(
        rotated(project_out),
        [(2 * share, w_out.shape[1] // 2)] * 2,
        attended,
        near,
        got,
        w_out,
        w_other,
        scratch=[pltpu.VMEM(twice, F32)],
    )
    (out,) = call(put_in_order, [(rows, w_out.shape[1] // 2)], kept, swapped(given))
    return out


def solution(mesh):
    placed = (
        P(("groups", "batch"), "seq"),
        P("seq"),
        P("seq", "head"),
        P(("groups", "batch"), "seq", None),
        P(("groups", "batch"), "seq", None),
        P(("groups", "batch"), None),
        P(("groups", "batch"), None),
        P(("groups", "batch")),
        P("head", "seq"),
    )
    return jax.shard_map(
        shards,
        mesh=mesh,
        in_specs=placed,
        out_specs=P(("groups", "batch"), ("seq", "head")),
        check_vma=False,
    )
```

```python
import functools

import jax
import jax.numpy as jnp
from jax import lax
from jax.experimental import pallas as pl
from jax.experimental.pallas import tpu as pltpu
from jax.sharding import PartitionSpec as P


HD = 128
QUAD = 4
FLOOR = -1e30
AHEAD = 20_000_000_000
F32 = jnp.float32
BF16 = jnp.bfloat16


def swapped(array):
    return lax.ppermute(array, "head", [(0, 1), (1, 0)])


def passed(block, targets):
    n, wide, cores = (lax.axis_size(a) for a in ("seq", "batch", "head"))
    pairs = []
    for i in range(n):
        for x in range(wide):
            for core, target in enumerate(targets):
                z, w = (i, x ^ 1) if target is None else (target(i) % n, x)
                pairs.append(((i * wide + x) * cores + core, (z * wide + w) * cores + core))
    return lax.ppermute(block, ("seq", "batch", "head"), pairs)


def inside(first, second):
    return [
        passed(first, (lambda i: i ^ 2, lambda i: i ^ 3)),
        passed(second, (None, lambda i: i ^ 1)),
    ]


def between(block):
    n = lax.axis_size("seq")
    return [
        passed(block, (lambda i: i + QUAD, lambda i: i + n // 2)),
        passed(block, (lambda i: i - QUAD, None)),
    ]


def call(kernel, shapes, *args, away=(), smem=(), scratch=(), mib=8, flops=0):
    def space(i):
        return pltpu.HBM if i in away else pltpu.SMEM if i in smem else pltpu.VMEM

    args = [
        pltpu.with_memory_space_constraint(a, pltpu.HBM) if i in away else a
        for i, a in enumerate(args)
    ]
    return pl.pallas_call(
        kernel,
        out_shape=[jax.ShapeDtypeStruct(s, F32) for s in shapes],
        in_specs=[pl.BlockSpec(memory_space=space(i)) for i in range(len(args))],
        out_specs=[pl.BlockSpec(memory_space=pltpu.VMEM) for _ in shapes],
        scratch_shapes=scratch,
        compiler_params=pltpu.CompilerParams(vmem_limit_bytes=mib << 20),
        cost_estimate=pl.CostEstimate(flops=flops, transcendentals=0, bytes_accessed=0)
        if flops
        else None,
    )(*args)


def core():
    return lax.axis_index("head")


def chosen():
    mine = lax.rem(lax.axis_index("seq"), QUAD)
    return mine ^ (2 + core()), mine ^ core()


def either(a_ref, b_ref):
    return jnp.where(core() == 1, b_ref[...], a_ref[...])


def project(x_hbm, g_hbm, w_hbm, part_ref, squares_ref, x_ref, g_ref, w_ref, sems):
    pairs = ((x_hbm, x_ref), (g_hbm, g_ref), (w_hbm, w_ref))
    copies = [pltpu.make_async_copy(a, b, sems.at[i]) for i, (a, b) in enumerate(pairs)]
    for copy in copies:
        copy.start()
    copies[0].wait()
    copies[1].wait()
    rows, width = x_ref.shape
    x = x_ref[...].astype(F32)
    squares = jnp.sum(x * x, axis=1, keepdims=True)
    squares_ref[...] = jnp.broadcast_to(squares, (rows, HD))
    scaled = x * g_ref[...].astype(F32).reshape(1, width)
    high = scaled.astype(BF16)
    low = (scaled - high.astype(F32)).astype(BF16)
    both = jnp.concatenate([high, low], axis=0)
    copies[2].wait()
    part = jnp.dot(both, w_ref[...], preferred_element_type=F32)
    part = part[:rows] + part[rows:]
    for b in range(rows):
        lines = [part[b : b + 1, h * HD : (h + 1) * HD] for h in range(part_ref.shape[1])]
        part_ref[b] = jnp.concatenate(lines, axis=0)


def assemble(own_ref, other_ref, squares_ref, first_ref, second_ref, chunk_ref):
    rows, half, _ = own_ref.shape
    heads = 2 * half
    share = rows // QUAD
    low = jnp.where(core() == 0, own_ref[...], other_ref[...])
    high = jnp.where(core() == 0, other_ref[...], own_ref[...])
    for b in range(rows):
        c, at = b // share, b % share * heads
        chunk_ref[c, at : at + half, :] = low[b]
        chunk_ref[c, at + half : at + heads, :] = high[b]
    squares = squares_ref[...]
    for c in range(QUAD):
        mine = squares[c * share : (c + 1) * share]
        chunk_ref[c, share * heads :, :] = jnp.concatenate([mine, mine], axis=0)
    for place, out_ref in zip(chosen(), (first_ref, second_ref), strict=True):
        out_ref[...] = chunk_ref[place]


def widen(w_ref, after_ref, out_ref):
    out_ref[...] = w_ref[...].astype(F32)


def rotated(kernel):
    def turned(a_ref, b_ref, first_ref, *refs):
        kernel(first_ref, a_ref, b_ref, *refs)

    return turned


def add_pair(a_ref, b_ref, out_ref):
    out_ref[...] = a_ref[...] + b_ref[...]


def add_either(got_ref, a_ref, b_ref, out_ref):
    out_ref[...] = got_ref[...] + either(a_ref, b_ref)


def finish_query(features, a_ref, b_ref, out_ref):
    total = a_ref[...] + b_ref[...]
    share, heads, _ = out_ref.shape
    scale = lax.rsqrt(total[share * heads :] / features + 1e-05) * (1.0 / HD**0.5)
    for i in range(share):
        mine = total[i * heads : (i + 1) * heads] * scale[i : i + 1]
        out_ref[i] = mine.astype(BF16).astype(F32)


def attend(first_ref, a_ref, b_ref, k_ref, v_ref, len_ref, *refs):
    *out_refs, q_ref, s_ref, top_ref = refs
    share, heads, _ = first_ref.shape
    q_ref[:share] = first_ref[...]
    q_ref[share:] = either(a_ref, b_ref)
    block = k_ref.shape[1]
    at = lax.axis_index("seq") * block + lax.broadcasted_iota(jnp.int32, (heads, block), 1)
    lane = lax.broadcasted_iota(jnp.int32, (heads, HD), 1)
    tops = jnp.zeros((heads, HD), F32)
    totals = jnp.zeros((heads, HD), F32)
    rows = [place * share + i for place in chosen() for i in range(share)]
    for j, b in enumerate(rows):
        q = q_ref[j].astype(BF16)
        s = lax.dot_general(q, k_ref[b], (((1,), (1,)), ((), ())), preferred_element_type=F32)
        s = jnp.where(at < len_ref[b], s, FLOOR)
        s_ref[j] = s
        top = jnp.maximum(jnp.max(s, axis=1, keepdims=True), FLOOR / 2)
        top_ref[j] = jnp.broadcast_to(top, (heads, HD))
        tops = jnp.where(lane == j, top, tops)
    for j, b in enumerate(rows):
        top = top_ref[j]
        weights = [jnp.exp(s_ref[j, :, i : i + HD] - top) for i in range(0, block, HD)]
        total = jnp.sum(functools.reduce(jnp.add, weights), axis=1, keepdims=True)
        totals = jnp.where(lane == j, total, totals)
        weights = jnp.concatenate([w.astype(BF16) for w in weights], axis=1)
        out_ref, i = out_refs[j // share], j % share
        out_ref[i * heads : (i + 1) * heads, :] = jnp.dot(
            weights, v_ref[b], preferred_element_type=F32
        )
    spare = jnp.zeros((HD - heads, HD), F32)
    tops = jnp.concatenate([tops, spare], axis=0).T
    totals = jnp.concatenate([totals, spare], axis=0).T
    for c, out_ref in enumerate(out_refs):
        mine = slice(c * share, (c + 1) * share)
        out_ref[share * heads :, :] = jnp.concatenate([tops[mine], totals[mine]], axis=0)


def joined(blocks, share, heads):
    at = share * heads
    tops = [r[at : at + share] for r in blocks]
    top = functools.reduce(jnp.maximum, tops)
    factors = [jnp.exp(t - top) for t in tops]
    total = functools.reduce(
        jnp.add, [f * r[at + share :] for f, r in zip(factors, blocks, strict=True)]
    )
    known = len(blocks) * share + 2 * share
    spare = jnp.zeros((HD - known, HD), F32)
    turned = jnp.concatenate([*factors, top, total, spare], axis=0).T[:heads]
    sums = []
    for i in range(share):
        parts = [
            turned[:, s * share + i : s * share + i + 1] * r[i * heads : (i + 1) * heads]
            for s, r in enumerate(blocks)
        ]
        sums.append(functools.reduce(jnp.add, parts))
    return sums, top, total, turned


def join(blocks, share, heads, out_ref):
    sums, top, total, _ = joined(blocks, share, heads)
    for i in range(share):
        out_ref[i * heads : (i + 1) * heads, :] = sums[i]
    out_ref[share * heads :, :] = jnp.concatenate([top, total], axis=0)


def join_pair(share, heads, a_ref, b_ref, out_ref):
    join([a_ref[...], b_ref[...]], share, heads, out_ref)


def join_either(share, heads, got_ref, a_ref, b_ref, out_ref):
    join([got_ref[...], either(a_ref, b_ref)], share, heads, out_ref)


def finish_attention(a_ref, b_ref, q_ref, knew_ref, vnew_ref, out_ref):
    share, heads, _ = out_ref.shape
    sums, _, _, turned = joined([a_ref[...], b_ref[...]], share, heads)
    known = 2 * share
    keys, values = knew_ref[...].astype(F32), vnew_ref[...].astype(F32)
    row = lax.broadcasted_iota(jnp.int32, keys.shape, 0)
    first = lax.rem(lax.axis_index("seq"), QUAD) * share
    for i in range(share):
        k_row = jnp.sum(jnp.where(row == first + i, keys, 0.0), axis=0, keepdims=True)
        v_row = jnp.sum(jnp.where(row == first + i, values, 0.0), axis=0, keepdims=True)
        own = jnp.sum(q_ref[i] * k_row, axis=1, keepdims=True)
        old = turned[:, known + i : known + i + 1]
        top = jnp.maximum(old, own)
        factor = jnp.exp(old - top)
        fresh = jnp.exp(own - top)
        total = factor * turned[:, known + share + i : known + share + i + 1] + fresh
        result = (factor * sums[i] + fresh * v_row) / total
        out_ref[i] = result.astype(BF16).astype(F32)


def project_out(first_ref, a_ref, b_ref, own_ref, other_ref, kept_ref, given_ref, all_ref):
    share, heads, _ = first_ref.shape
    all_ref[:share] = first_ref[...]
    all_ref[share:] = either(a_ref, b_ref)
    half = heads // 2
    zeroth = core() == 0
    low = jnp.concatenate([all_ref[:, h, :] for h in range(half)], axis=1)
    high = jnp.concatenate([all_ref[:, half + h, :] for h in range(half)], axis=1)
    own = jnp.where(zeroth, low, high).astype(BF16)
    other = jnp.where(zeroth, high, low).astype(BF16)
    out = jnp.dot(own, own_ref[...], preferred_element_type=F32)
    out += jnp.dot(other, other_ref[...].astype(BF16), preferred_element_type=F32)
    width = out.shape[1] // 2
    left, right = out[:, :width], out[:, width:]
    kept_ref[...] = jnp.where(zeroth, left, right)
    given_ref[...] = jnp.where(zeroth, right, left)


def put_in_order(kept_ref, got_ref, out_ref):
    share = kept_ref.shape[0] // 2
    far, near = chosen()
    kept, got = kept_ref[...], got_ref[...]
    lines = []
    for c in range(QUAD):
        mine = jnp.where(far == c, kept[:share], kept[share:])
        given = jnp.where((far ^ 1) == c, got[:share], got[share:])
        here = (far == c) | (near == c)
        lines.append(jnp.where(here, mine, given))
    out_ref[...] = jnp.concatenate(lines, axis=0)


def shards(
    hidden_in,
    norm_gain_vector,
    w_query,
    key_cache_rows,
    value_cache_rows,
    k_new,
    v_new,
    lengths,
    w_out,
):
    rows, width = hidden_in.shape
    half = w_query.shape[1] // HD
    heads = 2 * half
    n = lax.axis_size("seq")
    block = key_cache_rows.shape[1]
    share = rows // QUAD
    assert n == QUAD * QUAD and share * QUAD == rows and 2 * share == 8
    assert lax.axis_size("head") == 2 and lax.axis_size("batch") % 2 == 0 and heads <= HD
    chunk = (share * heads + 2 * share, HD)
    held = (share, heads, HD)
    twice = (2 * share, heads, HD)
    sizes = (share, heads)
    part, squares = call(
        project,
        [(rows, half, HD), (rows, HD)],
        hidden_in,
        norm_gain_vector,
        w_query,
        away=(0, 1, 2),
        scratch=[
            pltpu.VMEM(hidden_in.shape, BF16),
            pltpu.VMEM(norm_gain_vector.shape, BF16),
            pltpu.VMEM(w_query.shape, BF16),
            pltpu.SemaphoreType.DMA((3,)),
        ],
    )
    other = swapped(part)
    (wide,) = call(widen, [w_out.shape], w_out, squares)
    w_other = swapped(wide)
    first, second = call(
        assemble,
        [chunk] * 2,
        part,
        other,
        squares,
        scratch=[pltpu.VMEM((QUAD, *chunk), F32)],
    )
    got, near = inside(first, second)
    (mine,) = call(add_either, [chunk], got, second, near, flops=AHEAD)
    (mine,) = call(add_pair, [chunk], mine, swapped(mine))
    got, near = between(mine)
    (mine,) = call(rotated(add_either), [chunk], near, mine, got)
    finish = functools.partial(finish_query, width * n)
    (queries,) = call(finish, [held], mine, swapped(mine))
    got, near = inside(queries, queries)
    first, second = call(
        rotated(attend),
        [chunk] * 2,
        queries,
        near,
        got,
        key_cache_rows,
        value_cache_rows,
        lengths,
        smem=(5,),
        scratch=[
            pltpu.VMEM(twice, F32),
            pltpu.VMEM((2 * share, heads, block), F32),
            pltpu.VMEM(twice, F32),
        ],
    )
    got, near = inside(first, second)
    (mine,) = call(functools.partial(join_either, *sizes), [chunk], got, second, near)
    (mine,) = call(functools.partial(join_pair, *sizes), [chunk], mine, swapped(mine))
    got, near = between(mine)
    (mine,) = call(rotated(functools.partial(join_either, *sizes)), [chunk], near, mine, got)
    (attended,) = call(
        finish_attention, [held], mine, swapped(mine), queries, k_new, v_new
    )
    got, near = inside(attended, attended)
    kept, given = call(
        rotated(project_out),
        [(2 * share, w_out.shape[1] // 2)] * 2,
        attended,
        near,
        got,
        w_out,
        w_other,
        scratch=[pltpu.VMEM(twice, F32)],
    )
    (out,) = call(put_in_order, [(rows, w_out.shape[1] // 2)], kept, swapped(given))
    return out


def solution(mesh):
    placed = (
        P(("groups", "batch"), "seq"),
        P("seq"),
        P("seq", "head"),
        P(("groups", "batch"), "seq", None),
        P(("groups", "batch"), "seq", None),
        P(("groups", "batch"), None),
        P(("groups", "batch"), None),
        P(("groups", "batch")),
        P("head", "seq"),
    )
    return jax.shard_map(
        shards,
        mesh=mesh,
        in_specs=placed,
        out_specs=P(("groups", "batch"), ("seq", "head")),
        check_vma=False,
    )
```
